32 devices in a mesh: cfg: 2 (over y), ta: 4 (over z), sa: 2 (over x), src: 2 (over core).
Axes of the slice: x: 2, y: 2, z: 4, core: 2. Of those that a mesh axis runs over, the one named last changes fastest.
Arguments:
- prop: bfloat16 [4, 8, 2, 12, 12, 512], P(('cfg', 'src'), 'ta', None, None, None, 'sa'), parts along dimension 0, may hold values from -6 to 6
- eps_rows: int32 [24, 3], replicated, may hold values from 0 to 11
- eps_sign: int32 [24], replicated, may hold values from 0 to 1
- source_sites: int32 [4, 3], P('cfg'), parts along dimension 0, may hold values from 0 to 15, as said below
- momenta: int32 [8, 3], replicated, may hold values from -2 to 2
Outputs:
- blocks: float32 [4, 8, 2, 8, 1728], P('cfg', None, None, 'ta', 'sa'), parts along dimension 0
The draws below stay inside these ranges and needn't reach their ends.
There are 2 independent parts, one for each index of `cfg`. The reference program is written for one: setup_inputs(seed, part) draws one part's arguments, and reference() takes and returns one part's arrays. A program takes and returns all parts, laid end to end along the dimension named above; an argument that names none is the same for every part. Nothing has to cross between parts.
Inputs may be any that keep to these rules, and one draw needn't show every extreme that they name: `source_sites`: each row is a lattice site: first coordinate below 2, second below 16, third below 16.
All inputs are finite; a program needn't handle non-finite values.
Results may differ from the reference program's by a relative error of at most 0.0045.
Values sent between devices are 32-bit elements; how exact they have to be, the bound alone decides.
A program may use at most 128 MiB of HBM per device.

```python
import math
import jax
import jax.numpy as jnp
from jax import lax

SC = 12
TERMS = 24
LY = 16
LZ = 16
BLOCK = 1728
LX = 2
SITES = 512
TIMES = 8
NSRC = 2
MOM = 8


def draw_source_sites(key, part):
    key_x = jax.random.fold_in(key, 11)
    key_y = jax.random.fold_in(key, 12)
    key_z = jax.random.fold_in(key, 13)
    key_pick = jax.random.fold_in(key, 14)
    first = jax.random.randint(key_x, (NSRC,), 0, LX)
    second = jax.random.randint(key_y, (NSRC,), 0, LY)
    third = jax.random.randint(key_z, (NSRC,), 0, LZ)
    chosen = jax.random.randint(key_pick, (), 0, NSRC)
    follower = (chosen + 1) % NSRC
    rows = jnp.arange(NSRC, dtype=jnp.int32)
    corner = rows == chosen
    first = jnp.where(corner, LX - 1, first)
    second = jnp.where(corner, LY - 1, second)
    third = jnp.where(corner, LZ - 1, third)
    third = jnp.where(rows == follower, 0, third)
    return jnp.stack([first, second, third], axis=1).astype(jnp.int32)


def set_ends(entries, stream_key, least, top_value):
    longest = entries.shape.index(max(entries.shape))
    spots = []
    for shift in (0, 1):
        where = [jax.random.randint(jax.random.fold_in(stream_key, axis), (), 0, length) for axis, length in enumerate(entries.shape)]
        where[longest] = (where[longest] + shift) % entries.shape[longest]
        spots.append(tuple(where))
    return entries.at[spots[0]].set(least).at[spots[1]].set(top_value)


def shard_levels(stream_key, dims, shards, least, top_value):
    def one(axis_at, shards_of):
        steps = jax.random.uniform(jax.random.fold_in(jax.random.fold_in(stream_key, 6), axis_at), (shards_of,), jnp.float32, least / len(shards), top_value / len(shards))
        return jnp.repeat(jnp.exp(steps), dims[axis_at] // shards_of).reshape((-1,) + (1,) * (len(dims) - axis_at - 1))

    loudness = one(*shards[0])
    for cut in shards[1:]:
        loudness = loudness * one(*cut)
    return loudness


def normal_values(stream_key, dims, deviation, limit, pieces=(), kind=jnp.bfloat16):
    array = jax.random.normal(stream_key, dims, jnp.float32) * deviation
    if len(pieces) > 0:
        array = shard_levels(stream_key, dims, pieces, -0.22, 0.18) * array
    return jnp.clip(array, min=-limit, max=limit).astype(kind)


def setup_inputs(seed: int = 0, part: int = 0) -> dict:
    keys = jax.random.split(jax.random.key(seed), 6)
    part_splits = jax.random.split(jax.random.fold_in(keys[5], part), 6)
    return {
        "prop": normal_values(part_splits[0], (NSRC, TIMES, 2, SC, SC, SITES), 1.0, 6.0, ((0, 2), (1, 4), (5, 2))),
        "eps_rows": set_ends(jax.random.randint(keys[1], (TERMS, 3), 0, SC), jax.random.fold_in(keys[1], 1), 0, SC - 1).astype(jnp.int32),
        "eps_sign": set_ends(jax.random.randint(keys[2], (TERMS,), 0, 2), jax.random.fold_in(keys[2], 1), 0, 1).astype(jnp.int32),
        "source_sites": draw_source_sites(jax.random.fold_in(jax.random.fold_in(keys[5], part), 71), part),
        "momenta": set_ends(jax.random.randint(keys[4], (MOM, 3), -2, 3), jax.random.fold_in(keys[4], 1), -2, 2).astype(jnp.int32),
    }


def phase_table(position, momenta, site_index, extent_x):
    coord_x = site_index // (LY * LZ)
    coord_y = site_index // LZ % LY
    coord_z = site_index % LZ
    part_x = momenta[:, 0:1] * (coord_x[None, :] - position[0]) % extent_x
    part_y = momenta[:, 1:2] * (coord_y[None, :] - position[1]) % LY
    part_z = momenta[:, 2:3] * (coord_z[None, :] - position[2]) % LZ
    angle = 2.0 * math.pi * (part_x.astype(jnp.float32) / extent_x + part_y.astype(jnp.float32) / LY + part_z.astype(jnp.float32) / LZ)
    return jnp.concatenate([jnp.cos(angle), jnp.sin(angle)], axis=0).astype(jnp.bfloat16)

def contract(slab, rows, weights):
    first = jnp.take(slab, rows[:, 0], axis=1).astype(jnp.float32)
    second = jnp.take(slab, rows[:, 1], axis=1).astype(jnp.float32)
    third = jnp.take(slab, rows[:, 2], axis=1)
    scaled = weights[:, None, None, None]
    real = scaled * (first[0][:, :, None] * second[0][:, None] - first[1][:, :, None] * second[1][:, None])
    imag = scaled * (first[0][:, :, None] * second[1][:, None] + first[1][:, :, None] * second[0][:, None])
    pair = jnp.stack([real, imag]).astype(jnp.bfloat16)
    mixer = jnp.stack([jnp.stack([third[0], -third[1]]), jnp.stack([third[1], third[0]])])
    block = jnp.einsum('ceijx,oceLx->oijLx', pair.astype(jnp.float32), mixer.astype(jnp.float32))
    width = slab.shape[1]
    return block.astype(jnp.bfloat16).reshape(2 * width * width * width, slab.shape[-1])

def mix_phase(table, quark):
    product = jnp.dot(table, quark.T, preferred_element_type=jnp.float32)
    half_m = table.shape[0] // 2
    half_k = quark.shape[0] // 2
    cos_re = product[:half_m, :half_k]
    cos_im = product[:half_m, half_k:]
    sin_re = product[half_m:, :half_k]
    sin_im = product[half_m:, half_k:]
    return jnp.stack([cos_re + sin_im, cos_im - sin_re])

def reference(prop, eps_rows, eps_sign, source_sites, momenta):
    weights = (2 * eps_sign - 1).astype(jnp.float32)
    scale = 1.0 / math.sqrt(4.0 * TERMS * SITES)
    site_index = jnp.arange(SITES, dtype=jnp.int32)
    tables = jnp.stack([phase_table(source_sites[s], momenta, site_index, LX) for s in range(NSRC)])
    slabs = prop.reshape((NSRC * TIMES,) + prop.shape[2:])
    owners = jnp.repeat(jnp.arange(NSRC, dtype=jnp.int32), TIMES)

    def project(items):
        slab, owner = items
        quark = contract(slab, eps_rows, weights)
        return scale * mix_phase(tables[owner], quark)
    result = lax.map(project, (slabs, owners))
    return result.reshape(NSRC, TIMES, 2, MOM, BLOCK)
```

```python
import functools
import math

import jax
import jax.numpy as jnp
from jax import lax
from jax.experimental import pallas as pl
from jax.experimental.pallas import tpu as pltpu
from jax.sharding import PartitionSpec as P

LY = 16
LZ = 16
UNROLL = 4
F32 = jnp.float32
BF16 = jnp.bfloat16


def phase_rows(position, momenta, first_site, site_count, extent_x):
    site = first_site + lax.broadcasted_iota(jnp.int32, (1, site_count), 1)
    coords = (site // (LY * LZ), site // LZ % LY, site % LZ)
    turns = 0.0
    for axis, extent in enumerate((extent_x, LY, LZ)):
        steps = momenta[:, axis : axis + 1] * (coords[axis] - position[axis])
        part = steps & (extent - 1) if extent & (extent - 1) == 0 else steps % extent
        turns = turns + part.astype(F32) / extent
    angle = (2.0 * math.pi) * turns
    return jnp.cos(angle).astype(BF16).astype(F32), jnp.sin(angle).astype(BF16).astype(F32)


def compute_kernel(
    extent_x, scale, prop_ref, rows_ref, sign_ref, site_ref, mom_ref, out_ref,
    field, left, right, total, select,
):
    src_count, time_count, _, width, _, site_count = prop_ref.shape
    terms = rows_ref.shape[0]
    moms = mom_ref.shape[0]
    pad = field.shape[2]
    group = max(1, 16 // moms)
    first_site = lax.axis_index("sa") * site_count
    first_source = lax.axis_index("src") * src_count

    field[...] = jnp.zeros_like(field)
    spot = lax.broadcasted_iota(jnp.int32, select.shape, 0)
    column = lax.broadcasted_iota(jnp.int32, select.shape, 1)
    inner = spot % pad
    keep = (column == spot // pad * width + inner) & (inner < width)
    select[...] = jnp.where(keep, 1.0, 0.0).astype(BF16)

    def slab(source, time, cos, sin):
        for part in range(2):
            for row in range(width):
                field[part, row, 0:width, :] = prop_ref[source, time, part, row].astype(F32)

        @pl.loop(0, width)
        def _(row):
            for i in range(0, width, group):
                reals, imags = [], []
                for one in range(i, i + group):
                    re = field[0, row, one : one + 1, :]
                    im = field[1, row, one : one + 1, :]
                    reals.append(cos * re + sin * im)
                    imags.append(cos * im - sin * re)
                re = jnp.concatenate(reals, axis=0).astype(BF16)
                im = jnp.concatenate(imags, axis=0)
                upper = pl.ds(i * moms, group * moms)
                lower = pl.ds((width + i) * moms, group * moms)
                left[row, upper, 0:site_count] = re
                left[row, upper, site_count:] = (-im).astype(BF16)
                left[row, lower, 0:site_count] = im.astype(BF16)
                left[row, lower, site_count:] = re

        total[...] = jnp.zeros_like(total)

        @pl.loop(0, terms // UNROLL)
        def _(step):
            added = None
            for u in range(UNROLL):
                term = step * UNROLL + u
                weight = (2 * sign_ref[term] - 1).astype(F32)
                second = rows_ref[term, 1]
                third = rows_ref[term, 2]
                re = weight * field[0, third]
                im = weight * field[1, third]
                for j in range(width):
                    a = field[0, second, j : j + 1, :]
                    b = field[1, second, j : j + 1, :]
                    lines = pl.ds(j * pad, pad)
                    right[u, lines, 0:site_count] = (a * re - b * im).astype(BF16)
                    right[u, lines, site_count:] = (a * im + b * re).astype(BF16)
                product = lax.dot_general(
                    left[rows_ref[term, 0]], right[u], (((1,), (1,)), ((), ())),
                    preferred_element_type=F32,
                )
                added = product if added is None else added + product
            total[...] += added

        value = total[...] * scale
        high = value.astype(BF16)
        rest = value - high.astype(F32)
        middle = rest.astype(BF16)
        low = (rest - middle.astype(F32)).astype(BF16)
        dense = sum(
            jnp.dot(piece, select[...], preferred_element_type=F32)
            for piece in (low, middle, high)
        )
        for o in range(2):
            pieces = [
                dense[(o * width + i) * moms : (o * width + i + 1) * moms, :]
                for i in range(width)
            ]
            out_ref[source, time, o] = jnp.concatenate(pieces, axis=1)

    for source in range(src_count):
        position = [site_ref[first_source + source, axis] for axis in range(3)]
        cos, sin = phase_rows(position, mom_ref[...], first_site, site_count, extent_x)

        @pl.loop(0, time_count)
        def _(time):
            slab(source, time, cos, sin)


def partial_blocks(prop, eps_rows, eps_sign, source_sites, momenta):
    src_count, time_count, _, width, _, site_count = prop.shape
    sites_total = site_count * lax.axis_size("sa")
    extent_x = sites_total // (LY * LZ)
    scale = 1.0 / math.sqrt(4.0 * eps_rows.shape[0] * sites_total)
    moms = momenta.shape[0]
    pad = -(-width // 16) * 16
    vmem = pl.BlockSpec(memory_space=pltpu.VMEM)
    smem = pl.BlockSpec(memory_space=pltpu.SMEM)
    return pl.pallas_call(
        functools.partial(compute_kernel, extent_x, scale),
        out_shape=jax.ShapeDtypeStruct((src_count, time_count, 2, moms, width**3), F32),
        in_specs=[vmem, smem, smem, smem, vmem],
        out_specs=vmem,
        scratch_shapes=[
            pltpu.VMEM((2, width, pad, site_count), F32),
            pltpu.VMEM((width, 2 * width * moms, 2 * site_count), BF16),
            pltpu.VMEM((UNROLL, width * pad, 2 * site_count), BF16),
            pltpu.VMEM((2 * width * moms, width * pad), F32),
            pltpu.VMEM((width * pad, width * width), BF16),
        ],
        compiler_params=pltpu.CompilerParams(vmem_limit_bytes=48 * 1024 * 1024),
        name="blocks",
    )(prop, eps_rows, eps_sign, source_sites, momenta)


def per_device(prop, eps_rows, eps_sign, source_sites, momenta):
    ta, sa = lax.axis_size("ta"), lax.axis_size("sa")
    value = partial_blocks(prop, eps_rows, eps_sign, source_sites, momenta)
    src_count, time_count, _, moms, comps = value.shape
    value = value.reshape(src_count, time_count, 2, ta, moms // ta, sa, comps // sa)
    value = value.transpose(3, 5, 0, 1, 2, 4, 6).reshape(
        ta * sa, src_count, time_count, 2, moms // ta, comps // sa
    )
    value = lax.all_to_all(value, ("ta", "sa"), split_axis=0, concat_axis=0, tiled=True)
    value = value.reshape((ta, sa) + value.shape[1:]).sum(axis=1)
    value = value.transpose(1, 0, 2, 3, 4, 5).reshape(
        src_count, ta * time_count, 2, moms // ta, comps // sa
    )
    return lax.all_gather(value, "src", axis=0, tiled=True)


def solution(mesh):
    return jax.shard_map(
        per_device,
        mesh=mesh,
        in_specs=(P(("cfg", "src"), "ta", None, None, None, "sa"), P(), P(), P("cfg", None), P()),
        out_specs=P("cfg", None, None, "ta", "sa"),
        check_vma=False,
    )
```

```python
import functools
import math

import jax
import jax.numpy as jnp
from jax import lax
from jax.experimental import pallas as pl
from jax.experimental.pallas import tpu as pltpu
from jax.sharding import PartitionSpec as P

LY = 16
LZ = 16
UNROLL = 4
F32 = jnp.float32
BF16 = jnp.bfloat16


def phase_rows(position, momenta, first_site, site_count, extent_x):
    site = first_site + lax.broadcasted_iota(jnp.int32, (1, site_count), 1)
    coords = (site // (LY * LZ), site // LZ % LY, site % LZ)
    turns = 0.0
    for axis, extent in enumerate((extent_x, LY, LZ)):
        steps = momenta[:, axis : axis + 1] * (coords[axis] - position[axis])
        part = steps & (extent - 1) if extent & (extent - 1) == 0 else steps % extent
        turns = turns + part.astype(F32) / extent
    angle = (2.0 * math.pi) * turns
    return jnp.cos(angle).astype(BF16).astype(F32), jnp.sin(angle).astype(BF16).astype(F32)


def compute_kernel(
    extent_x, scale, prop_ref, rows_ref, sign_ref, site_ref, mom_ref, out_ref,
    field, left, right, total, select,
):
    src_count, time_count, _, width, _, site_count = prop_ref.shape
    terms = rows_ref.shape[0]
    moms = mom_ref.shape[0]
    pad = field.shape[2]
    group = max(1, 16 // moms)
    first_site = lax.axis_index("sa") * site_count
    first_source = lax.axis_index("src") * src_count
    sa_size, ta_size = out_ref.shape[:2]

    field[...] = jnp.zeros_like(field)
    spot = lax.broadcasted_iota(jnp.int32, select.shape, 0)
    column = lax.broadcasted_iota(jnp.int32, select.shape, 1)
    inner = spot % pad
    keep = (column == spot // pad * width + inner) & (inner < width)
    select[...] = jnp.where(keep, 1.0, 0.0).astype(BF16)

    def slab(source, time, cos, sin):
        for part in range(2):
            for row in range(width):
                field[part, row, 0:width, :] = prop_ref[source, time, part, row].astype(F32)

        @pl.loop(0, width)
        def _(row):
            for i in range(0, width, group):
                reals, imags = [], []
                for one in range(i, i + group):
                    re = field[0, row, one : one + 1, :]
                    im = field[1, row, one : one + 1, :]
                    reals.append(cos * re + sin * im)
                    imags.append(cos * im - sin * re)
                re = jnp.concatenate(reals, axis=0).astype(BF16)
                im = jnp.concatenate(imags, axis=0)
                upper = pl.ds(i * moms, group * moms)
                lower = pl.ds((width + i) * moms, group * moms)
                left[row, upper, 0:site_count] = re
                left[row, upper, site_count:] = (-im).astype(BF16)
                left[row, lower, 0:site_count] = im.astype(BF16)
                left[row, lower, site_count:] = re

        total[...] = jnp.zeros_like(total)

        @pl.loop(0, terms // UNROLL)
        def _(step):
            added = None
            for u in range(UNROLL):
                term = step * UNROLL + u
                weight = (2 * sign_ref[term] - 1).astype(F32)
                second = rows_ref[term, 1]
                third = rows_ref[term, 2]
                re = weight * field[0, third]
                im = weight * field[1, third]
                for j in range(width):
                    a = field[0, second, j : j + 1, :]
                    b = field[1, second, j : j + 1, :]
                    lines = pl.ds(j * pad, pad)
                    right[u, lines, 0:site_count] = (a * re - b * im).astype(BF16)
                    right[u, lines, site_count:] = (a * im + b * re).astype(BF16)
                product = lax.dot_general(
                    left[rows_ref[term, 0]], right[u], (((1,), (1,)), ((), ())),
                    preferred_element_type=F32,
                )
                added = product if added is None else added + product
            total[...] += added

        value = total[...] * scale
        high = value.astype(BF16)
        rest = value - high.astype(F32)
        middle = rest.astype(BF16)
        low = (rest - middle.astype(F32)).astype(BF16)
        dense = sum(
            jnp.dot(piece, select[...], preferred_element_type=F32)
            for piece in (low, middle, high)
        )
        share = width // sa_size
        each = moms // ta_size
        for o in range(2):
            line = ((source * time_count + time) * 2 + o) * each
            for piece in range(sa_size):
                lines = [
                    dense[(o * width + i) * moms : (o * width + i + 1) * moms, :]
                    for i in range(piece * share, (piece + 1) * share)
                ]
                lines = jnp.concatenate(lines, axis=1)
                for owner in range(ta_size):
                    out_ref[piece, owner, line : line + each, :] = lines[
                        owner * each : (owner + 1) * each
                    ]

    for source in range(src_count):
        position = [site_ref[first_source + source, axis] for axis in range(3)]
        cos, sin = phase_rows(position, mom_ref[...], first_site, site_count, extent_x)

        for time in range(time_count):
            slab(source, time, cos, sin)


def partial_blocks(prop, eps_rows, eps_sign, source_sites, momenta):
    src_count, time_count, _, width, _, site_count = prop.shape
    sa, ta = lax.axis_size("sa"), lax.axis_size("ta")
    sites_total = site_count * sa
    extent_x = sites_total // (LY * LZ)
    scale = 1.0 / math.sqrt(4.0 * eps_rows.shape[0] * sites_total)
    moms = momenta.shape[0]
    rows = src_count * time_count * 2 * moms // ta
    pad = -(-width // 16) * 16
    vmem = pl.BlockSpec(memory_space=pltpu.VMEM)
    smem = pl.BlockSpec(memory_space=pltpu.SMEM)
    return pl.pallas_call(
        functools.partial(compute_kernel, extent_x, scale),
        out_shape=jax.ShapeDtypeStruct((sa, ta, rows, width**3 // sa), F32),
        in_specs=[vmem, smem, smem, smem, vmem],
        out_specs=vmem,
        scratch_shapes=[
            pltpu.VMEM((2, width, pad, site_count), F32),
            pltpu.VMEM((width, 2 * width * moms, 2 * site_count), BF16),
            pltpu.VMEM((UNROLL, width * pad, 2 * site_count), BF16),
            pltpu.VMEM((2 * width * moms, width * pad), F32),
            pltpu.VMEM((width * pad, width * width), BF16),
        ],
        compiler_params=pltpu.CompilerParams(vmem_limit_bytes=48 * 1024 * 1024),
        name="blocks",
    )(prop, eps_rows, eps_sign, source_sites, momenta)


def exchange_kernel(part_ref, out_ref, landed, summed, done, send_x, recv_x, send_z, recv_z, send_c, recv_c):
    sa, ta = part_ref.shape[:2]
    src = done.shape[0]
    me_sa, me_ta, me_src = (lax.axis_index(name) for name in ("sa", "ta", "src"))

    def send(source, target, sems, device):
        copy = pltpu.make_async_remote_copy(
            src_ref=source, dst_ref=target, send_sem=sems[0], recv_sem=sems[1],
            device_id=device, device_id_type=pl.DeviceIdType.MESH,
        )
        copy.start()
        return copy

    barrier = pltpu.get_barrier_semaphore()
    peers = [{"sa": lax.rem(me_sa + d, sa)} for d in range(1, sa)]
    peers += [{"ta": lax.rem(me_ta + d, ta)} for d in range(1, ta)]
    peers += [{"src": lax.rem(me_src + d, src)} for d in range(1, src)]
    for peer in peers:
        pl.semaphore_signal(barrier, inc=1, device_id=peer, device_id_type=pl.DeviceIdType.MESH)
    pl.semaphore_wait(barrier, len(peers))

    order = list(range(1, ta)) + [0]
    owners = {d: lax.rem(me_ta + d, ta) for d in order}
    over_x = {}
    for d in order:
        for e in range(1, sa):
            target = lax.rem(me_sa + e, sa)
            over_x[d, e] = send(
                part_ref.at[target, owners[d]], landed.at[e - 1, d],
                (send_x.at[e - 1, d], recv_x.at[e - 1, d]), {"sa": target},
            )

    over_z = {}
    for d in order:
        value = part_ref[me_sa, owners[d]]
        for e in range(1, sa):
            over_x[d, e].wait_recv()
            value = value + landed[e - 1, d]
        if d == 0:
            done[me_src, me_ta] = value
        else:
            summed[d - 1] = value
            over_z[d] = send(
                summed.at[d - 1], done.at[me_src, me_ta],
                (send_z.at[d - 1], recv_z.at[d - 1]), {"ta": owners[d]},
            )

    over_c = {}
    for d in [0] + order[:-1]:
        origin = lax.rem(me_ta - d + ta, ta)
        if d:
            over_z[d].wait_recv()
        for e in range(1, src):
            over_c[d, e] = send(
                done.at[me_src, origin], done.at[me_src, origin],
                (send_c.at[e - 1, d], recv_c.at[e - 1, d]),
                {"src": lax.rem(me_src + e, src)},
            )
    for copy in over_c.values():
        copy.wait_recv()
    for copies in (over_x, over_z, over_c):
        for copy in copies.values():
            copy.wait_send()
    out_ref[...] = done[...]


def exchange(part):
    sa, ta, rows, comps = part.shape
    src = lax.axis_size("src")
    vmem = pl.BlockSpec(memory_space=pltpu.VMEM)
    pair = lambda *shape: [pltpu.SemaphoreType.DMA(shape)] * 2
    return pl.pallas_call(
        exchange_kernel,
        out_shape=jax.ShapeDtypeStruct((src, ta, rows, comps), F32),
        in_specs=[vmem],
        out_specs=vmem,
        scratch_shapes=[
            pltpu.VMEM((sa - 1, ta, rows, comps), F32),
            pltpu.VMEM((ta - 1, rows, comps), F32),
            pltpu.VMEM((src, ta, rows, comps), F32),
            *pair(sa - 1, ta), *pair(ta - 1), *pair(src - 1, ta),
        ],
        compiler_params=pltpu.CompilerParams(collective_id=0, has_side_effects=True),
        name="exchange",
    )(part)


def per_device(prop, eps_rows, eps_sign, source_sites, momenta):
    src_count, time_count = prop.shape[:2]
    done = exchange(partial_blocks(prop, eps_rows, eps_sign, source_sites, momenta))
    src, ta, rows, comps = done.shape
    done = done.reshape(src, ta, src_count, time_count, 2, -1, comps)
    done = done.transpose(0, 2, 1, 3, 4, 5, 6)
    return done.reshape(src * src_count, ta * time_count, 2, -1, comps)


def solution(mesh):
    return jax.shard_map(
        per_device,
        mesh=mesh,
        in_specs=(P(("cfg", "src"), "ta", None, None, None, "sa"), P(), P(), P("cfg", None), P()),
        out_specs=P("cfg", None, None, "ta", "sa"),
        check_vma=False,
    )
```

```python
import functools
import math

import jax
import jax.numpy as jnp
from jax import lax
from jax.experimental import pallas as pl
from jax.experimental.pallas import tpu as pltpu
from jax.sharding import PartitionSpec as P

LY = 16
LZ = 16
UNROLL = 4
F32 = jnp.float32
BF16 = jnp.bfloat16


def phase_rows(position, momenta, first_site, site_count, extent_x):
    site = first_site + lax.broadcasted_iota(jnp.int32, (1, site_count), 1)
    line = lax.broadcasted_iota(jnp.int32, (momenta.shape[1], site_count), 0)
    coords = (site // (LY * LZ), site // LZ % LY, site % LZ)
    turns = 0.0
    for axis, extent in enumerate((extent_x, LY, LZ)):
        factor = jnp.zeros_like(line)
        for mom in range(momenta.shape[1]):
            factor = jnp.where(line == mom, momenta[axis, mom], factor)
        steps = factor * (coords[axis] - position[axis])
        part = steps & (extent - 1) if extent & (extent - 1) == 0 else steps % extent
        turns = turns + part.astype(F32) / extent
    angle = (2.0 * math.pi) * turns
    return jnp.cos(angle).astype(BF16).astype(F32), jnp.sin(angle).astype(BF16).astype(F32)


def blocks_kernel(
    extent_x, scale, prop_ref, rows_ref, sign_ref, site_ref, mom_ref, out_ref,
    field, left, right, total, select, part_ref, landed, summed, done,
    send_x, recv_x, send_z, recv_z, send_c, recv_c,
):
    src_count, time_count, _, width, _, site_count = prop_ref.shape
    terms = rows_ref.shape[1]
    moms = mom_ref.shape[1]
    pad = field.shape[2]
    group = max(1, 16 // moms)
    first_site = lax.axis_index("sa") * site_count
    first_source = lax.axis_index("src") * src_count
    slabs, sa, ta = part_ref.shape[:3]
    src = done.shape[0]
    me_sa, me_ta, me_src = (lax.axis_index(name) for name in ("sa", "ta", "src"))

    barrier = pltpu.get_barrier_semaphore()
    peers = [{"sa": lax.rem(me_sa + d, sa)} for d in range(1, sa)]
    peers += [{"ta": lax.rem(me_ta + d, ta)} for d in range(1, ta)]
    peers += [{"src": lax.rem(me_src + d, src)} for d in range(1, src)]
    for peer in peers:
        pl.semaphore_signal(barrier, inc=1, device_id=peer, device_id_type=pl.DeviceIdType.MESH)

    field[...] = jnp.zeros_like(field)
    spot = lax.broadcasted_iota(jnp.int32, select.shape, 0)
    column = lax.broadcasted_iota(jnp.int32, select.shape, 1)
    inner = spot % pad
    keep = (column == spot // pad * width + inner) & (inner < width)
    select[...] = jnp.where(keep, 1.0, 0.0).astype(BF16)

    def slab(source, time, cos, sin):
        for part in range(2):
            for row in range(width):
                field[part, row, 0:width, :] = prop_ref[source, time, part, row].astype(F32)

        @pl.loop(0, width)
        def _(row):
            for i in range(0, width, group):
                reals, imags = [], []
                for one in range(i, i + group):
                    re = field[0, row, one : one + 1, :]
                    im = field[1, row, one : one + 1, :]
                    reals.append(cos * re + sin * im)
                    imags.append(cos * im - sin * re)
                re = jnp.concatenate(reals, axis=0).astype(BF16)
                im = jnp.concatenate(imags, axis=0)
                upper = pl.ds(i * moms, group * moms)
                lower = pl.ds((width + i) * moms, group * moms)
                left[row, upper, 0:site_count] = re
                left[row, upper, site_count:] = (-im).astype(BF16)
                left[row, lower, 0:site_count] = im.astype(BF16)
                left[row, lower, site_count:] = re

        total[...] = jnp.zeros_like(total)

        @pl.loop(0, terms // UNROLL)
        def _(step):
            added = None
            for u in range(UNROLL):
                term = step * UNROLL + u
                weight = (2 * sign_ref[term] - 1).astype(F32)
                second = rows_ref[1, term]
                third = rows_ref[2, term]
                re = weight * field[0, third]
                im = weight * field[1, third]
                for j in range(width):
                    a = field[0, second, j : j + 1, :]
                    b = field[1, second, j : j + 1, :]
                    lines = pl.ds(j * pad, pad)
                    right[u, lines, 0:site_count] = (a * re - b * im).astype(BF16)
                    right[u, lines, site_count:] = (a * im + b * re).astype(BF16)
                product = lax.dot_general(
                    left[rows_ref[0, term]], right[u], (((1,), (1,)), ((), ())),
                    preferred_element_type=F32,
                )
                added = product if added is None else added + product
            total[...] += added

        value = total[...] * scale
        high = value.astype(BF16)
        rest = value - high.astype(F32)
        middle = rest.astype(BF16)
        low = (rest - middle.astype(F32)).astype(BF16)
        dense = sum(
            jnp.dot(piece, select[...], preferred_element_type=F32)
            for piece in (low, middle, high)
        )
        share = width // sa
        each = moms // ta
        for o in range(2):
            for piece in range(sa):
                lines = [
                    dense[(o * width + i) * moms : (o * width + i + 1) * moms, :]
                    for i in range(piece * share, (piece + 1) * share)
                ]
                lines = jnp.concatenate(lines, axis=1)
                for owner in range(ta):
                    part_ref[source * time_count + time, piece, owner, o] = lines[
                        owner * each : (owner + 1) * each
                    ]

    def send(source, target, sems, device):
        copy = pltpu.make_async_remote_copy(
            src_ref=source, dst_ref=target, send_sem=sems[0], recv_sem=sems[1],
            device_id=device, device_id_type=pl.DeviceIdType.MESH,
        )
        copy.start()
        return copy

    order = list(range(1, ta)) + [0]
    owners = {d: lax.rem(me_ta + d, ta) for d in order}
    over_x, over_z, over_c = {}, {}, {}

    for source in range(src_count):
        position = [site_ref[first_source + source, axis] for axis in range(3)]
        cos, sin = phase_rows(position, mom_ref, first_site, site_count, extent_x)

        for time in range(time_count):
            slab(source, time, cos, sin)
            at = source * time_count + time
            if at == 0:
                pl.semaphore_wait(barrier, len(peers))
            for d in order:
                for e in range(1, sa):
                    target = lax.rem(me_sa + e, sa)
                    over_x[at, d, e] = send(
                        part_ref.at[at, target, owners[d]], landed.at[e - 1, at, d],
                        (send_x.at[e - 1, at, d], recv_x.at[e - 1, at, d]), {"sa": target},
                    )

    for at in range(slabs):
        for d in order:
            value = part_ref[at, me_sa, owners[d]]
            for e in range(1, sa):
                over_x[at, d, e].wait_recv()
                value = value + landed[e - 1, at, d]
            if d == 0:
                done[me_src, me_ta, at] = value
            else:
                summed[d - 1, at] = value
                over_z[at, d] = send(
                    summed.at[d - 1, at], done.at[me_src, me_ta, at],
                    (send_z.at[d - 1, at], recv_z.at[d - 1, at]), {"ta": owners[d]},
                )

    for at in range(slabs):
        for d in [0] + order[:-1]:
            origin = lax.rem(me_ta - d + ta, ta)
            if d:
                over_z[at, d].wait_recv()
            for e in range(1, src):
                over_c[at, d, e] = send(
                    done.at[me_src, origin, at], done.at[me_src, origin, at],
                    (send_c.at[e - 1, at, d], recv_c.at[e - 1, at, d]),
                    {"src": lax.rem(me_src + e, src)},
                )
    for copy in over_c.values():
        copy.wait_recv()
    for copies in (over_x, over_z, over_c):
        for copy in copies.values():
            copy.wait_send()
    out_ref[...] = done[...]


def per_device(prop, eps_rows, eps_sign, source_sites, momenta):
    src_count, time_count, _, width, _, site_count = prop.shape
    sa, ta, src = (lax.axis_size(name) for name in ("sa", "ta", "src"))
    sites_total = site_count * sa
    extent_x = sites_total // (LY * LZ)
    scale = 1.0 / math.sqrt(4.0 * eps_rows.shape[0] * sites_total)
    moms = momenta.shape[0]
    each, comps, slabs = moms // ta, width**3 // sa, src_count * time_count
    pad = -(-width // 16) * 16
    vmem = pl.BlockSpec(memory_space=pltpu.VMEM)
    smem = pl.BlockSpec(memory_space=pltpu.SMEM)
    pair = lambda *shape: [pltpu.SemaphoreType.DMA(shape)] * 2
    done = pl.pallas_call(
        functools.partial(blocks_kernel, extent_x, scale),
        out_shape=jax.ShapeDtypeStruct((src, ta, slabs, 2, each, comps), F32),
        in_specs=[vmem, smem, smem, smem, smem],
        out_specs=vmem,
        scratch_shapes=[
            pltpu.VMEM((2, width, pad, site_count), F32),
            pltpu.VMEM((width, 2 * width * moms, 2 * site_count), BF16),
            pltpu.VMEM((UNROLL, width * pad, 2 * site_count), BF16),
            pltpu.VMEM((2 * width * moms, width * pad), F32),
            pltpu.VMEM((width * pad, width * width), BF16),
            pltpu.VMEM((slabs, sa, ta, 2, each, comps), F32),
            pltpu.VMEM((sa - 1, slabs, ta, 2, each, comps), F32),
            pltpu.VMEM((ta - 1, slabs, 2, each, comps), F32),
            pltpu.VMEM((src, ta, slabs, 2, each, comps), F32),
            *pair(sa - 1, slabs, ta), *pair(ta - 1, slabs), *pair(src - 1, slabs, ta),
        ],
        compiler_params=pltpu.CompilerParams(
            vmem_limit_bytes=48 * 1024 * 1024, collective_id=0, has_side_effects=True
        ),
        name="blocks",
    )(prop, eps_rows.T, eps_sign, source_sites, momenta.T)
    done = done.reshape(src, ta, src_count, time_count, 2, each, comps)
    done = done.transpose(0, 2, 1, 3, 4, 5, 6)
    return done.reshape(src * src_count, ta * time_count, 2, each, comps)


def solution(mesh):
    return jax.shard_map(
        per_device,
        mesh=mesh,
        in_specs=(P(("cfg", "src"), "ta", None, None, None, "sa"), P(), P(), P("cfg", None), P()),
        out_specs=P("cfg", None, None, "ta", "sa"),
        check_vma=False,
    )
```
